32 devices in a mesh: rows: 8 (over z, y), cols: 4 (over x, core).
Axes of the slice: x: 2, y: 2, z: 4, core: 2. Of those that a mesh axis runs over, the one named last changes fastest.
Arguments:
- features: bfloat16 [64, 512, 512], P('rows', 'cols'), may hold values from -6 to 6
- dw_weight: float32 [49, 512], replicated, may hold values from -0.875 to 0.875
- norm_gain: float32 [512], replicated, may hold values from 0.1 to 1.9
- w_up: bfloat16 [512, 2048], replicated, may hold values from -0.25 to 0.25
- w_down: bfloat16 [2048, 512], replicated, may hold values from -0.125 to 0.125
- cotangent: bfloat16 [64, 512, 512], P('rows', 'cols'), may hold values from -6 to 6
Outputs:
- grad_input: bfloat16 [64, 512, 512], P('rows', 'cols')
- grad_dw: float32 [49, 512], replicated
- grad_gain: float32 [512], replicated
- grad_up: float32 [512, 2048], replicated
- grad_down: float32 [2048, 512], replicated
The draws below stay inside these ranges and needn't reach their ends.
All inputs are finite; a program needn't handle non-finite values.
Results may differ from the reference program's by a relative error of at most 0.019.
Values may be sent and summed in bfloat16 or wider, within the bound.
No kernel may reach another device: no remote copies, remote signals or barrier semaphores. Data moves between devices by JAX's collectives and lax.ppermute only.
A program may use at most 128 MiB of HBM per device.

```python
import jax
import jax.numpy as jnp
from jax import lax

C = 512
FF = 2048
KK = 49
H = 64
W = 512


def shard_levels(stream_key, shape, split, smallest, largest):
    level, own = 1.0, jax.random.fold_in(stream_key, 6)
    for dim, parts in split:
        steps = jnp.exp(jax.random.uniform(jax.random.fold_in(own, dim), (parts,), jnp.float32, smallest / len(split), largest / len(split)))
        level = level * jnp.repeat(steps, shape[dim] // parts).reshape([-1 if axis == dim else 1 for axis in range(len(shape))])
    return level


def normal_values(rng, dims, scale, bound, split=(), kind=jnp.bfloat16):
    values = jax.random.normal(rng, dims, jnp.float32) * scale
    if len(split) > 0:
        values = shard_levels(rng, dims, split, -0.22, 0.18) * values
    return jnp.clip(values, min=-bound, max=bound).astype(kind)


def setup_inputs(seed: int = 0) -> dict:
    keys = jax.random.split(jax.random.key(seed), 7)
    features = normal_values(keys[0], (H, W, C), 1.0, 6.0, ((0, 8), (1, 4)))
    dw_weight = normal_values(keys[1], (KK, C), KK ** -0.5, 0.875, (), jnp.float32)
    norm_gain = jnp.clip(1.0 + 0.18 * jax.random.normal(keys[2], (C,), jnp.float32), 0.1, 1.9)
    w_up = normal_values(keys[3], (C, FF), C ** -0.5, 0.25)
    w_down = normal_values(keys[4], (FF, C), FF ** -0.5, 0.125)
    cotangent = normal_values(keys[5], (H, W, C), 1.0, 6.0, ((0, 8), (1, 4)))
    return {"features": features, "dw_weight": dw_weight, "norm_gain": norm_gain, "w_up": w_up, "w_down": w_down, "cotangent": cotangent}


eps = 1e-06

def depthwise(padded, weight, rows, cols):
    total = jnp.zeros((rows, cols, padded.shape[2]), jnp.float32)
    for tap_i in range(7):
        for tap_j in range(7):
            total = total + padded[tap_i:tap_i + rows, tap_j:tap_j + cols] * weight[7 * tap_i + tap_j]
    return total

def pointwise(conv, gain, w_up, w_down, grad_out):
    mean = lax.optimization_barrier(jnp.mean(conv, axis=-1, keepdims=True))
    centred = conv - mean
    inv = lax.rsqrt(lax.optimization_barrier(jnp.mean(centred * centred, axis=-1, keepdims=True)) + eps)
    normed = centred * inv
    scaled = (normed * gain).astype(jnp.bfloat16)
    hidden = jnp.dot(scaled, w_up, preferred_element_type=jnp.float32)
    act = (0.5 * hidden * (1.0 + lax.erf(hidden * 0.7071067811865476))).astype(jnp.bfloat16)
    grad_down = lax.dot_general(act, grad_out, (((0,), (0,)), ((), ())), preferred_element_type=jnp.float32)
    grad_act = lax.dot_general(grad_out, w_down, (((1,), (1,)), ((), ())), preferred_element_type=jnp.float32)
    slope = 0.5 * (1.0 + lax.erf(hidden * 0.7071067811865476)) + hidden * jnp.exp(-0.5 * hidden * hidden) * 0.3989422804014327
    grad_hidden = (grad_act * slope).astype(jnp.bfloat16)
    grad_up = lax.dot_general(scaled, grad_hidden, (((0,), (0,)), ((), ())), preferred_element_type=jnp.float32)
    grad_scaled = lax.dot_general(grad_hidden, w_up, (((1,), (1,)), ((), ())), preferred_element_type=jnp.float32)
    grad_gain = lax.optimization_barrier(jnp.sum(grad_scaled * normed, axis=0))
    g_norm = grad_scaled * gain
    grad_conv = inv * (g_norm - lax.optimization_barrier(jnp.mean(g_norm, axis=-1, keepdims=True)) - normed * lax.optimization_barrier(jnp.mean(g_norm * normed, axis=-1, keepdims=True)))
    return (grad_conv.astype(jnp.bfloat16), grad_up, grad_down, grad_gain)

def reference(features, dw_weight, norm_gain, w_up, w_down, cotangent):
    padded = jnp.pad(features.astype(jnp.float32), ((3, 3), (3, 3), (0, 0)))
    conv = depthwise(padded, dw_weight, H, W)
    blocks = H // 8
    conv_blocks = conv.reshape(blocks, 8 * W, C)
    grad_blocks = cotangent.reshape(blocks, 8 * W, C)

    def step(carry, pair):
        grad_conv, grad_up, grad_down, grad_gain = pointwise(pair[0], norm_gain, w_up, w_down, pair[1])
        return ((carry[0] + grad_up, carry[1] + grad_down, carry[2] + grad_gain), grad_conv)
    start = (jnp.zeros((C, FF), jnp.float32), jnp.zeros((FF, C), jnp.float32), jnp.zeros((C,), jnp.float32))
    sums, grad_conv = lax.scan(step, start, (conv_blocks, grad_blocks))
    grad_conv = grad_conv.reshape(H, W, C)
    grad_f = grad_conv.astype(jnp.float32)
    taps = []
    for tap_i in range(7):
        for tap_j in range(7):
            taps.append(lax.optimization_barrier(jnp.sum(padded[tap_i:tap_i + H, tap_j:tap_j + W] * grad_f, axis=(0, 1))))
    grad_dw = jnp.stack(taps)
    grad_pad = jnp.pad(grad_f, ((3, 3), (3, 3), (0, 0)))
    total = cotangent.astype(jnp.float32)
    for tap_i in range(7):
        for tap_j in range(7):
            total = total + grad_pad[6 - tap_i:6 - tap_i + H, 6 - tap_j:6 - tap_j + W] * dw_weight[7 * tap_i + tap_j]
    return (total.astype(jnp.bfloat16), grad_dw, sums[2], sums[0], sums[1])
```

```python
import functools
import jax, jax.numpy as jnp
from jax import lax
from jax.sharding import PartitionSpec as P
from jax.experimental import pallas as pl
from jax.experimental.pallas import tpu as pltpu
bf16, f32 = jnp.bfloat16, jnp.float32
VM = pl.BlockSpec(memory_space=pltpu.VMEM)
PADC = 8

def fill(xs, x_ref, top, bot, lft, rgt, ctop, cbot, r, c, nb):
    def put(row0, nrow, col0, ref):
        ncol = ref.shape[1]
        for b in range(nb):
            xs[row0:row0 + nrow, b, col0:col0 + ncol, :] = ref[:, :, b * 128:(b + 1) * 128].astype(f32)
    put(3, r, PADC, x_ref)
    put(0, 3, PADC, top)
    put(r + 3, 3, PADC, bot)
    put(3, r, PADC - 3, lft)
    put(3, r, PADC + c, rgt)
    for b in range(nb):
        s = slice(b * 128, (b + 1) * 128)
        xs[0:3, b, PADC - 3:PADC, :] = ctop[:, 0:3, s].astype(f32)
        xs[0:3, b, PADC + c:PADC + c + 3, :] = ctop[:, 3:6, s].astype(f32)
        xs[r + 3:r + 6, b, PADC - 3:PADC, :] = cbot[:, 0:3, s].astype(f32)
        xs[r + 3:r + 6, b, PADC + c:PADC + c + 3, :] = cbot[:, 3:6, s].astype(f32)

def conv_into(out, xs, w_ref, r, c, nb, flip, base=None, unroll=2):
    def body(t, _):
        b = t // (c // (8 * unroll))
        k = t % (c // (8 * unroll))
        c0 = pl.multiple_of(k * (8 * unroll), 8 * unroll)
        lane = pl.multiple_of(b * 128, 128)
        acc = [[None] * unroll for _ in range(r)]
        if base is not None:
            for o in range(r):
                blk = base[o, pl.ds(c0, 8 * unroll), pl.ds(lane, 128)].astype(f32)
                for u in range(unroll):
                    acc[o][u] = blk[8 * u:8 * u + 8]
        for j in range(7):
            ws = []
            for i in range(7):
                tap = 7 * i + j
                if flip: tap = 48 - tap
                ws.append(jnp.broadcast_to(w_ref[tap:tap + 1, pl.ds(lane, 128)], (8, 128)))
            for q in range(r + 6):
                for u in range(unroll):
                    v = xs[q, b, pl.ds(c0 + 8 * u + PADC - 3 + j, 8), :]
                    for i in range(7):
                        o = q - i
                        if 0 <= o < r:
                            p = v * ws[i]
                            acc[o][u] = p if acc[o][u] is None else acc[o][u] + p
        for o in range(r):
            blk = jnp.concatenate(acc[o], axis=0)
            out[o, pl.ds(c0, 8 * unroll), pl.ds(lane, 128)] = blk.astype(out.dtype)
        return 0
    lax.fori_loop(0, nb * (c // (8 * unroll)), body, 0)

def fwd_kernel(x_ref, top, bot, lft, rgt, ctop, cbot, w_ref, gain, scaled, scaled_t, normed, inv_ref, xs):
    r, c, ch = x_ref.shape
    nb = ch // 128
    fill(xs, x_ref, top, bot, lft, rgt, ctop, cbot, r, c, nb)
    conv_into(normed, xs, w_ref, r, c, nb, False)
    g = gain[...]
    def ln(t, _):
        o = t
        x = normed[o]
        mean = jnp.mean(x, axis=-1, keepdims=True)
        cen = x - mean
        inv = lax.rsqrt(jnp.mean(cen * cen, axis=-1, keepdims=True) + 1e-6)
        nrm = cen * inv
        normed[o] = nrm
        inv_ref[o] = jnp.broadcast_to(inv, (c, 128))
        sc = (nrm * g).astype(bf16)
        scaled[o] = sc
        scaled_t[:, pl.ds(pl.multiple_of(o * c, c), c)] = sc.T
        return 0
    lax.fori_loop(0, r, ln, 0)

def forward(x, top, bot, lft, rgt, ctop, cbot, w, gain):
    r, c, ch = x.shape
    S = jax.ShapeDtypeStruct
    return pl.pallas_call(
        fwd_kernel,
        out_shape=(S((r, c, ch), bf16), S((ch, r * c), bf16), S((r, c, ch), f32), S((r, c, 128), f32)),
        in_specs=[VM] * 9, out_specs=(VM,) * 4,
        scratch_shapes=[pltpu.VMEM((r + 6, ch // 128, c + 16, 128), f32)],
        compiler_params=pltpu.CompilerParams(vmem_limit_bytes=48 << 20),
        name="conv_norm",
    )(x, top, bot, lft, rgt, ctop, cbot, w, gain)

NT = (((1,), (1,)), ((), ()))
def mlp_kernel(scaled, scaled_t, cot, cot_t, w_up, w_down, gd, gu, gh_out, *, fc):
    ff = w_up.shape[1]
    def body(k, _):
        f0 = pl.multiple_of(k * fc, fc)
        h = jnp.dot(scaled[...], w_up[:, pl.ds(f0, fc)], preferred_element_type=f32)
        ga = lax.dot_general(cot[...], w_down[pl.ds(f0, fc), :], NT, preferred_element_type=f32)
        phi = 0.5 + 0.5 * lax.erf(h * 0.7071067811865476)
        act = (h * phi).astype(bf16)
        slope = phi + h * (jnp.exp(-0.5 * h * h) * 0.3989422804014327)
        gh = (ga * slope).astype(bf16)
        gh_out[:, pl.ds(f0, fc)] = gh
        gd[:, pl.ds(f0, fc)] = jnp.dot(cot_t[...], act, preferred_element_type=f32).astype(gd.dtype)
        gu[:, pl.ds(f0, fc)] = jnp.dot(scaled_t[...], gh, preferred_element_type=f32).astype(gu.dtype)
        return 0
    lax.fori_loop(0, ff // fc, body, 0)

def mlp(scaled, scaled_t, cot, cot_t, w_up, w_down, fc=256):
    n, ch = scaled.shape
    ff = w_up.shape[1]
    S = jax.ShapeDtypeStruct
    return pl.pallas_call(
        functools.partial(mlp_kernel, fc=fc),
        out_shape=(S((ch, ff), bf16), S((ch, ff), bf16), S((n, ff), bf16)),
        in_specs=[VM] * 6, out_specs=(VM,) * 3,
        compiler_params=pltpu.CompilerParams(vmem_limit_bytes=48 << 20),
        name="mlp",
    )(scaled, scaled_t, cot, cot_t, w_up, w_down)

def back_kernel(gh, w_up, normed, inv_ref, gain, gc, gg):
    n, ch = normed.shape
    rb = 256
    g = gain[...]
    def body(k, tot):
        r0 = pl.multiple_of(k * rb, rb)
        gs = lax.dot_general(gh[pl.ds(r0, rb), :], w_up[...], NT, preferred_element_type=f32)
        nrm = normed[pl.ds(r0, rb), :]
        inv = inv_ref[pl.ds(r0, rb), 0:1]
        gn = gs * nrm
        tot = tot + jnp.sum(gn.reshape(rb // 8, 8, ch), axis=0)
        m1 = jnp.mean(gs * g, axis=-1, keepdims=True)
        m2 = jnp.mean(gn * g, axis=-1, keepdims=True)
        gc[pl.ds(r0, rb), :] = (inv * (gs * g - m1 - nrm * m2)).astype(bf16)
        return tot
    tot = lax.fori_loop(0, n // rb, body, jnp.zeros((8, ch), f32))
    gg[...] = jnp.sum(tot, axis=0, keepdims=True)

def back(gh, w_up, normed, inv, gain):
    n, ch = normed.shape
    S = jax.ShapeDtypeStruct
    return pl.pallas_call(
        back_kernel, out_shape=(S((n, ch), bf16), S((1, ch), f32)),
        in_specs=[VM] * 5, out_specs=(VM,) * 2,
        compiler_params=pltpu.CompilerParams(vmem_limit_bytes=48 << 20), name="norm_back",
    )(gh, w_up, normed, inv, gain)

def taps_kernel(x_ref, top, bot, lft, rgt, ctop, cbot, gc, gg, dw, xs, gf):
    r, c, ch = x_ref.shape
    nb = ch // 128
    fill(xs, x_ref, top, bot, lft, rgt, ctop, cbot, r, c, nb)
    dw[...] = jnp.zeros(dw.shape, dw.dtype)
    for b in range(nb):
        gf[:, b] = gc[:, :, b * 128:(b + 1) * 128].astype(f32)
    def body(b, _):
        lane = pl.multiple_of(b * 128, 128)
        for j in range(7):
            def inner(k, acc):
                c0 = pl.multiple_of(k * 8, 8)
                gs = [gf[o, b, pl.ds(c0, 8), :] for o in range(r)]
                acc = list(acc)
                for q in range(r + 6):
                    v = xs[q, b, pl.ds(c0 + PADC - 3 + j, 8), :]
                    for i in range(7):
                        o = q - i
                        if 0 <= o < r:
                            acc[i] = acc[i] + v * gs[o]
                return tuple(acc)
            acc = lax.fori_loop(0, c // 8, inner, tuple(jnp.zeros((8, 128), f32) for _ in range(7)), unroll=4)
            for i in range(7):
                tap = 7 * i + j
                dw[tap:tap + 1, pl.ds(lane, 128)] = jnp.sum(acc[i], axis=0, keepdims=True)
        return 0
    lax.fori_loop(0, nb, body, 0)
    dw[49:50, :] = gg[...]

def taps(x, top, bot, lft, rgt, ctop, cbot, gc, gg):
    r, c, ch = x.shape
    S = jax.ShapeDtypeStruct
    return pl.pallas_call(
        taps_kernel, out_shape=S((56, ch), f32), in_specs=[VM] * 9, out_specs=VM,
        scratch_shapes=[pltpu.VMEM((r + 6, ch // 128, c + 16, 128), f32), pltpu.VMEM((r, ch // 128, c, 128), f32)],
        compiler_params=pltpu.CompilerParams(vmem_limit_bytes=48 << 20), name="tap_sums",
    )(x, top, bot, lft, rgt, ctop, cbot, gc, gg)

def spread_kernel(x_ref, top, bot, lft, rgt, ctop, cbot, w_ref, cot, out, xs):
    r, c, ch = x_ref.shape
    nb = ch // 128
    fill(xs, x_ref, top, bot, lft, rgt, ctop, cbot, r, c, nb)
    conv_into(out, xs, w_ref, r, c, nb, True, base=cot)

def spread(x, top, bot, lft, rgt, ctop, cbot, w, cot):
    r, c, ch = x.shape
    return pl.pallas_call(
        spread_kernel, out_shape=jax.ShapeDtypeStruct((r, c, ch), bf16), in_specs=[VM] * 9, out_specs=VM,
        scratch_shapes=[pltpu.VMEM((r + 6, ch // 128, c + 16, 128), f32)],
        compiler_params=pltpu.CompilerParams(vmem_limit_bytes=48 << 20), name="spread",
    )(x, top, bot, lft, rgt, ctop, cbot, w, cot)


def ring_shift(block, axis, step):
    count = lax.axis_size(axis)
    pairs = [(i, i + step) for i in range(count) if 0 <= i + step < count]
    return lax.ppermute(block, axis, pairs)


def halo(block):
    r, c = block.shape[:2]
    lft = ring_shift(block[:, c - 3:], "cols", 1)
    rgt = ring_shift(block[:, :3], "cols", -1)
    top = ring_shift(block[r - 3:], "rows", 1)
    bot = ring_shift(block[:3], "rows", -1)
    side = jnp.concatenate([lft, rgt], axis=1)
    ctop = ring_shift(side[r - 3:], "rows", 1)
    cbot = ring_shift(side[:3], "rows", -1)
    return block, top, bot, lft, rgt, ctop, cbot


def bits_of(axis):
    count = lax.axis_size(axis)
    assert count & (count - 1) == 0
    return [(axis, 1 << k) for k in range(count.bit_length() - 1)]


def swap(block, axis, bit):
    return lax.ppermute(block, axis, [(i, i ^ bit) for i in range(lax.axis_size(axis))])


def side_of(axis, bit):
    return (lax.axis_index(axis) // bit) % 2


def total_sum(block, order):
    for axis, bit in order:
        half = block.shape[0] // 2
        side = side_of(axis, bit)
        keep = lax.dynamic_slice_in_dim(block, side * half, half, 0)
        send = lax.dynamic_slice_in_dim(block, (1 - side) * half, half, 0)
        got = swap(send, axis, bit)
        block = (keep.astype(f32) + got.astype(f32)).astype(bf16)
    for axis, bit in reversed(order):
        side = side_of(axis, bit)
        got = swap(block, axis, bit)
        low = jnp.where(side == 0, block, got)
        high = jnp.where(side == 0, got, block)
        block = jnp.concatenate([low, high], axis=0)
    return block


def small_sum(block, order):
    for axis, bit in order:
        mine = block.astype(bf16)
        block = mine.astype(f32) + swap(mine, axis, bit).astype(f32)
    return block


def on_device(features, dw_weight, norm_gain, w_up, w_down, cotangent):
    r, c, ch = features.shape
    n = r * c
    gain = norm_gain.reshape(1, ch)
    cot = cotangent.reshape(n, ch)
    padded = halo(features)
    scaled, scaled_t, normed, inv = forward(*padded, dw_weight, gain)
    gd_t, gu, gh = mlp(scaled.reshape(n, ch), scaled_t, cot, cot.T, w_up, w_down)
    cols, rows = bits_of("cols"), bits_of("rows")
    gd_t = total_sum(gd_t, cols + rows)
    gu = total_sum(gu, cols[:1] + rows + cols[1:])
    gc, gg = back(gh, w_up, normed.reshape(n, ch), inv.reshape(n, 128), gain)
    gc = gc.reshape(r, c, ch)
    wide = halo(gc)
    small = taps(*padded, gc, gg)
    small = small_sum(small, cols + rows)
    grad_input = spread(*wide, dw_weight, cotangent)
    return (grad_input, small[:49], small[49], gu.astype(f32), gd_t.T.astype(f32))


def solution(mesh):
    tile, whole = P("rows", "cols", None), P()
    return jax.shard_map(
        on_device,
        mesh=mesh,
        in_specs=(tile, whole, whole, whole, whole, tile),
        out_specs=(tile, whole, whole, whole, whole),
        check_vma=False,
    )
```
